8 devices in a mesh: data: 1 (over z), tp: 2 (over y), cp: 4 (over x, core).
Axes of the slice: x: 2, y: 2, z: 1, core: 2. Of those that a mesh axis runs over, the one named last changes fastest.
Arguments:
- x: bfloat16 [16, 1024, 8192], P('data', ('cp', 'tp'))
- positions: int32 [16, 1024], P('data', ('cp', 'tp'))
- w_query: bfloat16 [8192, 8192], P(None, 'tp')
- w_key: bfloat16 [8192, 8192], P(None, 'tp')
- w_value: bfloat16 [8192, 8192], P(None, 'tp')
- w_out: bfloat16 [8192, 8192], P('tp')
Outputs:
- output: bfloat16 [16, 1024, 8192], P('data', ('cp', 'tp'))
All inputs are finite; a program needn't handle non-finite values.
Results may differ from the reference program's by a relative error of at most 0.00652.
Values are sent between devices in bfloat16 or wider.
A program may use at most 1.5 GiB of HBM per device.

```python
import math
import jax
import jax.numpy as jnp
from jax import lax

BATCH_ROWS = 16
CHUNK_LEN = 128
CP_SIZE = 4
MODEL_DIM = 8192
Q_HEADS = 64
KV_HEADS = 64
HEAD_DIM = 128
ROPE_BASE = 500000
WALK_RANK = 64
SEQ_LEN = 2 * CP_SIZE * CHUNK_LEN
Q_PER_KV = Q_HEADS // KV_HEADS
N_BLOCKS = SEQ_LEN // CHUNK_LEN


def to_storage_order(seq_vals):
    trailing = seq_vals.shape[2:]
    blocks = seq_vals.reshape((seq_vals.shape[0], 2 * CP_SIZE, CHUNK_LEN) + trailing)
    first_half = blocks[:, :CP_SIZE]
    second_half = jnp.flip(blocks[:, CP_SIZE:], axis=1)
    return jnp.stack([first_half, second_half], axis=2).reshape(seq_vals.shape)


def setup_inputs(seed: int = 0, part: int = 0) -> dict:
    part_key = jax.random.fold_in(jax.random.key(seed), part)
    draw_keys = jax.random.split(part_key, 5)
    weight_keys = jax.random.split(jax.random.key(seed + 1), 4)
    common = jax.random.normal(draw_keys[0], (BATCH_ROWS, 1, MODEL_DIM), jnp.float32)
    walk_steps = jax.random.normal(draw_keys[1], (BATCH_ROWS, SEQ_LEN, WALK_RANK), jnp.float32)
    walk_path = jnp.cumsum(walk_steps, axis=1) / math.sqrt(SEQ_LEN)
    walk_basis = jax.random.normal(draw_keys[2], (WALK_RANK, MODEL_DIM), jnp.float32) / math.sqrt(WALK_RANK)
    noise_part = jax.random.normal(draw_keys[3], (BATCH_ROWS, SEQ_LEN, MODEL_DIM), jnp.float32)
    x_seq = 0.5 * common + 0.8 * jnp.einsum('bsr,rd->bsd', walk_path, walk_basis) + 0.5 * noise_part
    pos_gaps = jax.random.randint(draw_keys[4], (BATCH_ROWS, SEQ_LEN), 1, 5, dtype=jnp.int32)
    pos_seq = jnp.cumsum(pos_gaps, axis=1, dtype=jnp.int32) - 1
    q_scale = 2.0 / math.sqrt(MODEL_DIM)
    in_scale = 1.0 / math.sqrt(MODEL_DIM)
    out_scale = 1.0 / math.sqrt(Q_HEADS * HEAD_DIM)
    w_query = jax.random.normal(weight_keys[0], (MODEL_DIM, Q_HEADS * HEAD_DIM), jnp.float32) * q_scale
    w_key = jax.random.normal(weight_keys[1], (MODEL_DIM, KV_HEADS * HEAD_DIM), jnp.float32) * in_scale
    w_value = jax.random.normal(weight_keys[2], (MODEL_DIM, KV_HEADS * HEAD_DIM), jnp.float32) * in_scale
    w_out = jax.random.normal(weight_keys[3], (Q_HEADS * HEAD_DIM, MODEL_DIM), jnp.float32) * out_scale
    return {
        'x': to_storage_order(x_seq).astype(jnp.bfloat16),
        'positions': to_storage_order(pos_seq),
        'w_query': w_query.astype(jnp.bfloat16),
        'w_key': w_key.astype(jnp.bfloat16),
        'w_value': w_value.astype(jnp.bfloat16),
        'w_out': w_out.astype(jnp.bfloat16),
    }


def rope_tables(pos_vals):
    inv_freq = jnp.asarray([ROPE_BASE ** (-2.0 * freq_idx / HEAD_DIM) for freq_idx in range(HEAD_DIM // 2)], dtype=jnp.float32)
    angles = pos_vals.astype(jnp.float32)[..., None] * inv_freq
    return jnp.cos(angles), jnp.sin(angles)


def apply_rope(head_vals, cos_t, sin_t):
    half_dim = head_vals.shape[-1] // 2
    lower_half = head_vals[..., :half_dim]
    upper_half = head_vals[..., half_dim:]
    return jnp.concatenate([lower_half * cos_t - upper_half * sin_t, upper_half * cos_t + lower_half * sin_t], axis=-1)


def attend_sequence(row_args):
    q_row, k_row, v_row, pos_row = row_args
    k_blocks = k_row.astype(jnp.float32).reshape(N_BLOCKS, CHUNK_LEN, KV_HEADS, HEAD_DIM)
    v_blocks = v_row.astype(jnp.float32).reshape(N_BLOCKS, CHUNK_LEN, KV_HEADS, HEAD_DIM)
    kpos_blocks = pos_row.reshape(N_BLOCKS, CHUNK_LEN)
    score_scale = 1.0 / math.sqrt(HEAD_DIM)

    def query_block(query_args):
        q_blk, qpos_blk = query_args
        q_f32 = q_blk.astype(jnp.float32)

        def block_scores(k_blk, kpos_blk):
            raw_scores = jnp.einsum('qhgd,khd->hgqk', q_f32, k_blk) * score_scale
            visible = kpos_blk[None, :] <= qpos_blk[:, None]
            return jnp.where(visible, raw_scores, -jnp.inf)

        def max_step(run_max, key_args):
            k_blk, kpos_blk = key_args
            return jnp.maximum(run_max, block_scores(k_blk, kpos_blk).max(axis=-1)), None

        init_max = jnp.full((KV_HEADS, Q_PER_KV, CHUNK_LEN), -jnp.inf, jnp.float32)
        row_max, _ = lax.scan(max_step, init_max, (k_blocks, kpos_blocks))

        def sum_step(loop_carry, key_args):
            run_sum, out_accum = loop_carry
            k_blk, v_blk, kpos_blk = key_args
            exp_scores = jnp.exp(block_scores(k_blk, kpos_blk) - row_max[..., None])
            rounded = exp_scores.astype(jnp.bfloat16).astype(jnp.float32)
            out_accum = out_accum + jnp.einsum('hgqk,khd->hgqd', rounded, v_blk)
            return (run_sum + exp_scores.sum(axis=-1), out_accum), None

        init_sum = jnp.zeros((KV_HEADS, Q_PER_KV, CHUNK_LEN), jnp.float32)
        init_accum = jnp.zeros((KV_HEADS, Q_PER_KV, CHUNK_LEN, HEAD_DIM), jnp.float32)
        (row_sum, out_accum), _ = lax.scan(sum_step, (init_sum, init_accum), (k_blocks, v_blocks, kpos_blocks))
        normed = (out_accum / row_sum[..., None]).astype(jnp.bfloat16)
        return jnp.transpose(normed, (2, 0, 1, 3)).reshape(CHUNK_LEN, Q_HEADS * HEAD_DIM)

    q_blocks = q_row.reshape(N_BLOCKS, CHUNK_LEN, KV_HEADS, Q_PER_KV, HEAD_DIM)
    out_blocks = lax.map(query_block, (q_blocks, pos_row.reshape(N_BLOCKS, CHUNK_LEN)))
    return out_blocks.reshape(SEQ_LEN, Q_HEADS * HEAD_DIM)


def reference(x, positions, w_query, w_key, w_value, w_out):
    flat_x = x.reshape(BATCH_ROWS * SEQ_LEN, MODEL_DIM)
    q_proj = jnp.dot(flat_x, w_query, preferred_element_type=jnp.float32).astype(jnp.bfloat16)
    k_proj = jnp.dot(flat_x, w_key, preferred_element_type=jnp.float32).astype(jnp.bfloat16)
    v_proj = jnp.dot(flat_x, w_value, preferred_element_type=jnp.float32).astype(jnp.bfloat16)
    cos_t, sin_t = rope_tables(positions)
    q_heads = q_proj.reshape(BATCH_ROWS, SEQ_LEN, KV_HEADS, Q_PER_KV, HEAD_DIM).astype(jnp.float32)
    q_rot = apply_rope(q_heads, cos_t[:, :, None, None, :], sin_t[:, :, None, None, :]).astype(jnp.bfloat16)
    k_heads = k_proj.reshape(BATCH_ROWS, SEQ_LEN, KV_HEADS, HEAD_DIM).astype(jnp.float32)
    k_rot = apply_rope(k_heads, cos_t[:, :, None, :], sin_t[:, :, None, :]).astype(jnp.bfloat16)
    v_heads = v_proj.reshape(BATCH_ROWS, SEQ_LEN, KV_HEADS, HEAD_DIM)
    attn_out = lax.map(attend_sequence, (q_rot, k_rot, v_heads, positions))
    out_proj = jnp.dot(attn_out.reshape(BATCH_ROWS * SEQ_LEN, Q_HEADS * HEAD_DIM), w_out, preferred_element_type=jnp.float32)
    return (x.astype(jnp.float32) + out_proj.reshape(BATCH_ROWS, SEQ_LEN, MODEL_DIM)).astype(jnp.bfloat16)
```

```python
import functools
import math
import jax
import jax.numpy as jnp
from jax import lax
from jax.experimental import pallas as pl
from jax.experimental.pallas import tpu as pltpu
from jax.sharding import PartitionSpec as P

HEAD_DIM = 128
ROPE_BASE = 500000
Q_TILE = 256
STEP_HEADS = 2
EXP_SCALE = math.log2(math.e) / math.sqrt(HEAD_DIM)
W_PIECES = 2


def rope_tables(pos_vals):
    inv_freq = jnp.asarray([ROPE_BASE ** (-2.0 * freq_idx / HEAD_DIM) for freq_idx in range(HEAD_DIM // 2)], dtype=jnp.float32)
    angles = pos_vals.astype(jnp.float32)[..., None] * inv_freq
    cos_t, sin_t = jnp.cos(angles), jnp.sin(angles)
    return jnp.concatenate([cos_t, cos_t], axis=-1), jnp.concatenate([-sin_t, sin_t], axis=-1)


def attend_kernel(place_ref, q_ref, k_ref, v_ref, cos_ref, sin_ref, o_ref, q_seq, k_seq, v_seq):
    n_rows = q_ref.shape[0]
    n_chunks = place_ref.shape[1]
    chunk = n_rows // n_chunks
    n_heads = q_ref.shape[1] // HEAD_DIM
    for m in range(n_chunks):
        src = slice(m * chunk, (m + 1) * chunk)
        dst = pl.ds(pl.multiple_of(place_ref[0, m] * chunk, chunk), chunk)
        cos_t, sin_t = cos_ref[src, :], sin_ref[src, :]
        for h in range(n_heads):
            cols = slice(h * HEAD_DIM, (h + 1) * HEAD_DIM)
            for in_ref, out_ref in ((q_ref, q_seq), (k_ref, k_seq)):
                vals = in_ref[src, cols].astype(jnp.float32)
                out_ref[dst, cols] = (vals * cos_t + pltpu.roll(vals, HEAD_DIM // 2, 1) * sin_t).astype(jnp.bfloat16)
        v_seq[dst, :] = v_ref[src, :]
    tile = min(Q_TILE, n_rows)
    below = lax.broadcasted_iota(jnp.int32, (tile, tile), 1) <= lax.broadcasted_iota(jnp.int32, (tile, tile), 0)
    contract_last = (((1,), (1,)), ((), ()))
    for j in range(n_rows // tile):
        for h in range(n_heads):
            cols = slice(h * HEAD_DIM, (h + 1) * HEAD_DIM)
            here = slice(j * tile, (j + 1) * tile)
            q_tile = q_seq[here, cols]
            s_diag = lax.dot_general(q_tile, k_seq[here, cols], contract_last, preferred_element_type=jnp.float32)
            s_diag = jnp.where(below, s_diag, -jnp.inf)
            row_max = jnp.max(s_diag, axis=1, keepdims=True)
            if j:
                s_prev = lax.dot_general(q_tile, k_seq[:j * tile, cols], contract_last, preferred_element_type=jnp.float32)
                row_max = jnp.maximum(row_max, jnp.max(s_prev, axis=1, keepdims=True))
            p_diag = jnp.exp2((s_diag - row_max) * EXP_SCALE)
            row_sum = jnp.sum(p_diag, axis=1, keepdims=True)
            acc = jnp.dot(p_diag.astype(jnp.bfloat16), v_seq[here, cols], preferred_element_type=jnp.float32)
            if j:
                p_prev = jnp.exp2((s_prev - row_max) * EXP_SCALE)
                row_sum = row_sum + jnp.sum(p_prev, axis=1, keepdims=True)
                acc = acc + jnp.dot(p_prev.astype(jnp.bfloat16), v_seq[:j * tile, cols], preferred_element_type=jnp.float32)
            out = (acc / row_sum).astype(jnp.bfloat16)
            for part in range(tile // chunk):
                dst = pl.ds(pl.multiple_of(place_ref[1, j * (tile // chunk) + part] * chunk, chunk), chunk)
                o_ref[dst, cols] = out[part * chunk:(part + 1) * chunk]


def attend(place, q, k, v, cos_t, sin_t):
    n_rows, width = q.shape
    step_w = STEP_HEADS * HEAD_DIM
    head_spec = pl.BlockSpec((n_rows, step_w), lambda g, place_ref: (0, g))
    table_spec = pl.BlockSpec((n_rows, HEAD_DIM), lambda g, place_ref: (0, 0))
    flops = 2 * n_rows * n_rows * width
    return pl.pallas_call(
        attend_kernel,
        out_shape=jax.ShapeDtypeStruct((n_rows, width), jnp.bfloat16),
        grid_spec=pltpu.PrefetchScalarGridSpec(
            num_scalar_prefetch=1, grid=(width // step_w,),
            in_specs=[head_spec] * 3 + [table_spec] * 2, out_specs=head_spec,
            scratch_shapes=[pltpu.VMEM((n_rows, step_w), jnp.bfloat16)] * 3),
        compiler_params=pltpu.CompilerParams(dimension_semantics=('arbitrary',), vmem_limit_bytes=48 * 2 ** 20),
        cost_estimate=pl.CostEstimate(flops=8 * flops, bytes_accessed=8 * n_rows * width, transcendentals=n_rows * n_rows * width // HEAD_DIM),
        name='attend',
    )(place, q, k, v, cos_t, sin_t)


def out_kernel(n_w, n_peers, tp_size, cp_ref, *refs):
    w_refs, pieces = refs[:n_w], refs[n_w:n_w + n_peers]
    x_ref = refs[n_w + n_peers]
    y_ref, o_all, sems = refs[-3:]
    chunk, width = pieces[0].shape
    cp_i = cp_ref[0]
    cp_size = n_peers // tp_size
    part_w = width // cp_size

    @pl.when(pl.program_id(0) == 0)
    def _():
        copies = []
        for m, piece in enumerate(pieces):
            mc, mt = m // tp_size, m % tp_size
            rows = pl.ds(pl.multiple_of((cp_i ^ mc) * chunk, chunk), chunk)
            if mt == 0:
                copies.append((piece, o_all.at[rows, pl.ds(0, width)]))
                continue
            for part in range(cp_size):
                cols = pl.ds(pl.multiple_of((cp_i ^ part) * part_w, part_w), part_w)
                copies.append((piece.at[:, cols], o_all.at[rows, pl.ds(width + part * part_w, part_w)]))
        copies = [pltpu.make_async_copy(src, dst, sems.at[n]) for n, (src, dst) in enumerate(copies)]
        for copy in copies:
            copy.start()
        for copy in copies:
            copy.wait()

    first, acc = 0, None
    for w_ref in w_refs:
        depth = w_ref.shape[0]
        term = jnp.dot(o_all[:, first:first + depth], w_ref[...], preferred_element_type=jnp.float32)
        acc = term if acc is None else acc + term
        first += depth
    y_ref[...] = (x_ref[...].astype(jnp.float32) + acc).astype(jnp.bfloat16)


def out_project(cp_i, w_parts, pieces, x_flat, y_buf, s, tp_size, n_tile=512):
    chunk, width = pieces[0].shape
    n_rows = chunk * len(pieces) // tp_size
    depth = width * tp_size
    dim = x_flat.shape[1]
    n_tile = min(n_tile, dim)
    any_spec = pl.BlockSpec(memory_space=pl.ANY)
    row_spec = pl.BlockSpec((n_rows, n_tile), lambda g, cp_ref: (s, g))
    operands = [*w_parts, *pieces, x_flat]
    in_specs = [pl.BlockSpec((w.shape[0], n_tile), lambda g, cp_ref: (0, g)) for w in w_parts] + [any_spec] * len(pieces) + [row_spec]
    aliases = {}
    if y_buf is not None:
        aliases = {1 + len(operands): 0}
        operands.append(y_buf)
        in_specs.append(any_spec)
    return pl.pallas_call(
        functools.partial(out_kernel, len(w_parts), len(pieces), tp_size),
        out_shape=jax.ShapeDtypeStruct(x_flat.shape, jnp.bfloat16),
        grid_spec=pltpu.PrefetchScalarGridSpec(
            num_scalar_prefetch=1, grid=(dim // n_tile,), in_specs=in_specs, out_specs=row_spec,
            scratch_shapes=[pltpu.VMEM((n_rows, depth), jnp.bfloat16), pltpu.SemaphoreType.DMA((len(pieces) * len(pieces),))]),
        input_output_aliases=aliases,
        compiler_params=pltpu.CompilerParams(dimension_semantics=('arbitrary',), vmem_limit_bytes=48 * 2 ** 20),
        cost_estimate=pl.CostEstimate(flops=2 * n_rows * depth * dim, bytes_accessed=2 * depth * dim + 2 * n_rows * (depth + 2 * dim), transcendentals=0),
        name='out_project',
    )(cp_i, *operands)


def solution(mesh):
    cp_size, tp_size = mesh.shape['cp'], mesh.shape['tp']
    n_peers = cp_size * tp_size
    row_spec = P('data', ('cp', 'tp'))

    def swap(vals, m):
        if not m:
            return vals
        mc, mt = m // tp_size, m % tp_size
        pairs = [(t * cp_size + c, (t ^ mt) * cp_size + (c ^ mc)) for t in range(tp_size) for c in range(cp_size)]
        return lax.ppermute(vals, ('tp', 'cp'), pairs)

    def local_fn(x_rows, pos_rows, w_query, w_key, w_value, w_out):
        n_seqs, chunk, dim = x_rows.shape
        n_own = n_seqs // cp_size
        cp_i, tp_i = lax.axis_index('cp'), lax.axis_index('tp')
        me = cp_i * tp_size + tp_i
        peers = me ^ jnp.arange(n_peers, dtype=jnp.int32)
        peer_cp, peer_tp = peers // tp_size, peers % tp_size
        block_of = jnp.where(peer_tp == 0, peer_cp, 2 * cp_size - 1 - peer_cp)
        chunk_of = jnp.argmax(block_of[None, :] == jnp.arange(n_peers, dtype=jnp.int32)[:, None], axis=1).astype(jnp.int32)
        place = jnp.stack([block_of, chunk_of]).astype(jnp.int32)
        pos_all = lax.all_gather(pos_rows, ('tp', 'cp'), axis=0, tiled=False)
        pos_all = jnp.take(pos_all, peer_tp * cp_size + peer_cp, axis=0)

        def seq_of(s, mc):
            return s * cp_size + (cp_i ^ mc)

        seq_x = []
        for s in range(n_own):
            outgoing = [lax.dynamic_index_in_dim(x_rows, seq_of(s, mc), 0, keepdims=False) for mc in range(cp_size)]
            seq_x.append([swap(outgoing[m // tp_size], m) for m in range(n_peers)])

        q_rows = w_out.shape[0] // cp_size
        piece_rows = q_rows // W_PIECES
        w_got = [[None] * W_PIECES for _ in range(cp_size)]
        for p in range(W_PIECES):
            mine = lax.dynamic_slice_in_dim(w_out, cp_i * q_rows + p * piece_rows, piece_rows, 0)
            w_got[0][p] = swap(mine, 1)
            w_got[1][p] = swap(w_got[0][p], tp_size)
            w_got[2][p] = swap(w_got[0][p], 2 * tp_size)
            w_got[3][p] = swap(w_got[2][p], tp_size)
        w_parts = [w_out] + [piece for part in w_got for piece in part]

        o_got = []
        for s in range(n_own):
            x_seq = jnp.concatenate(seq_x[s], axis=0)
            pos_seq = lax.dynamic_index_in_dim(pos_all, seq_of(s, 0), 1, keepdims=False).reshape(-1)
            cos_t, sin_t = rope_tables(pos_seq)
            q, k, v = [jnp.dot(x_seq, w, preferred_element_type=jnp.float32).astype(jnp.bfloat16) for w in (w_query, w_key, w_value)]
            o = attend(place, q, k, v, cos_t, sin_t)
            o_got.append([swap(o[m * chunk:(m + 1) * chunk], m) for m in range(n_peers)])

        x_flat = x_rows.reshape(n_seqs * chunk, dim)
        y = None
        for s in range(n_own):
            y = out_project(cp_i.reshape(1).astype(jnp.int32), w_parts, o_got[s], x_flat, y, s, tp_size)
        return y.reshape(n_seqs, chunk, dim)


    return jax.shard_map(local_fn, mesh=mesh,
                         in_specs=(row_spec, row_spec, P(None, 'tp'), P(None, 'tp'), P(None, 'tp'), P('tp', None)),
                         out_specs=row_spec, check_vma=False)
```

```python
import functools
import math
import jax
import jax.numpy as jnp
from jax import lax
from jax.experimental import pallas as pl
from jax.experimental.pallas import tpu as pltpu
from jax.sharding import PartitionSpec as P

HEAD_DIM = 128
ROPE_BASE = 500000
Q_TILE = 256
STEP_HEADS = 2
EXP_SCALE = math.log2(math.e) / math.sqrt(HEAD_DIM)
W_PIECES = 2
QKV_TILE = 512
OUT_TILE = 512
CP_SIZE = 4
OWN = 4
NEAR = (0, 2)


def rope_tables(pos_vals):
    inv_freq = jnp.asarray([ROPE_BASE ** (-2.0 * freq_idx / HEAD_DIM) for freq_idx in range(HEAD_DIM // 2)], dtype=jnp.float32)
    angles = pos_vals.astype(jnp.float32)[..., None] * inv_freq
    cos_t, sin_t = jnp.cos(angles), jnp.sin(angles)
    return jnp.concatenate([cos_t, cos_t], axis=-1), jnp.concatenate([-sin_t, sin_t], axis=-1)


def attend_kernel(sources, place_ref, *refs):
    n_chunks = place_ref.shape[1]
    qkv_refs, (cos_ref, sin_ref) = refs[:6], refs[6:8]
    o_refs, (q_seq, k_seq, v_seq, o_seq) = refs[8:8 + n_chunks], refs[8 + n_chunks:]
    n_rows, step_w = q_seq.shape
    chunk = n_rows // n_chunks
    heads = [slice(h * HEAD_DIM, (h + 1) * HEAD_DIM) for h in range(step_w // HEAD_DIM)]
    for m, (which, first) in enumerate(sources):
        q_ref, k_ref, v_ref = qkv_refs[which::2]
        src, tab = slice(first, first + chunk), slice(m * chunk, (m + 1) * chunk)
        dst = pl.ds(pl.multiple_of(place_ref[0, m] * chunk, chunk), chunk)
        cos_t, sin_t = cos_ref[tab, :], sin_ref[tab, :]
        for cols in heads:
            for in_ref, out_ref in ((q_ref, q_seq), (k_ref, k_seq)):
                vals = in_ref[src, cols].astype(jnp.float32)
                out_ref[dst, cols] = (vals * cos_t + pltpu.roll(vals, HEAD_DIM // 2, 1) * sin_t).astype(jnp.bfloat16)
        v_seq[dst, :] = v_ref[src, :]
    tile = min(Q_TILE, n_rows)
    below = lax.broadcasted_iota(jnp.int32, (tile, tile), 1) <= lax.broadcasted_iota(jnp.int32, (tile, tile), 0)
    contract_last = (((1,), (1,)), ((), ()))
    for j in range(n_rows // tile):
        for cols in heads:
            here = slice(j * tile, (j + 1) * tile)
            q_tile = q_seq[here, cols]
            s_diag = lax.dot_general(q_tile, k_seq[here, cols], contract_last, preferred_element_type=jnp.float32)
            s_diag = jnp.where(below, s_diag, -jnp.inf)
            row_max = jnp.max(s_diag, axis=1, keepdims=True)
            if j:
                s_prev = lax.dot_general(q_tile, k_seq[:j * tile, cols], contract_last, preferred_element_type=jnp.float32)
                row_max = jnp.maximum(row_max, jnp.max(s_prev, axis=1, keepdims=True))
            p_diag = jnp.exp2((s_diag - row_max) * EXP_SCALE)
            row_sum = jnp.sum(p_diag, axis=1, keepdims=True)
            acc = jnp.dot(p_diag.astype(jnp.bfloat16), v_seq[here, cols], preferred_element_type=jnp.float32)
            if j:
                p_prev = jnp.exp2((s_prev - row_max) * EXP_SCALE)
                row_sum = row_sum + jnp.sum(p_prev, axis=1, keepdims=True)
                acc = acc + jnp.dot(p_prev.astype(jnp.bfloat16), v_seq[:j * tile, cols], preferred_element_type=jnp.float32)
            o_seq[here, cols] = (acc / row_sum).astype(jnp.bfloat16)
    for m, o_ref in enumerate(o_refs):
        o_ref[...] = o_seq[pl.ds(pl.multiple_of(place_ref[0, m] * chunk, chunk), chunk), :]


def attend(place, qkv_near, qkv_far, s, near, cos_t, sin_t):
    n_rows, n_peers = cos_t.shape[0], place.shape[1]
    chunk = n_rows // n_peers
    width = qkv_far.shape[1] // 3
    step_w = STEP_HEADS * HEAD_DIM
    steps = width // step_w
    near_rows = len(near) * chunk
    far = [m for m in range(n_peers) if m not in near]
    sources = [(0, near.index(m) * chunk) if m in near else (1, far.index(m) * chunk) for m in range(n_peers)]
    qkv_specs = []
    for part in range(3):
        qkv_specs.append(pl.BlockSpec((near_rows, step_w), lambda g, place_ref, part=part: (s, part * steps + g)))
        qkv_specs.append(pl.BlockSpec((len(far) * chunk, step_w), lambda g, place_ref, part=part: (0, part * steps + g)))
    table_spec = pl.BlockSpec((n_rows, HEAD_DIM), lambda g, place_ref: (0, 0))
    out_spec = pl.BlockSpec((chunk, step_w), lambda g, place_ref: (0, g))
    flops = 2 * n_rows * n_rows * width
    return pl.pallas_call(
        functools.partial(attend_kernel, sources),
        out_shape=[jax.ShapeDtypeStruct((chunk, width), jnp.bfloat16)] * n_peers,
        grid_spec=pltpu.PrefetchScalarGridSpec(
            num_scalar_prefetch=1, grid=(steps,),
            in_specs=qkv_specs + [table_spec] * 2, out_specs=[out_spec] * n_peers,
            scratch_shapes=[pltpu.VMEM((n_rows, step_w), jnp.bfloat16)] * 4),
        compiler_params=pltpu.CompilerParams(dimension_semantics=('arbitrary',), vmem_limit_bytes=48 * 2 ** 20),
        cost_estimate=pl.CostEstimate(flops=4 * flops, bytes_accessed=8 * n_rows * width, transcendentals=n_rows * n_rows * width // HEAD_DIM // 2),
        name='attend',
    )(place, *[qkv_near, qkv_far] * 3, cos_t, sin_t)


def fetch_all(copies, sems):
    copies = [pltpu.make_async_copy(src, dst, sems.at[n]) for n, (src, dst) in enumerate(copies)]
    for copy in copies:
        copy.start()
    return copies


def qkv_kernel(n_rows_in, picks, cp_ref, *refs):
    rows_in, w_refs = refs[:n_rows_in], refs[n_rows_in:n_rows_in + 3]
    out_ref, x_all, w_buf, w_sems, x_sems = refs[n_rows_in + 3:]
    step, last = pl.program_id(0), pl.num_programs(0) - 1
    n_tile = w_buf.shape[2]
    per_w = w_refs[0].shape[1] // n_tile

    def fetch(index, act):
        slot = lax.rem(index, 2)
        for part, w_ref in enumerate(w_refs):
            @pl.when(lax.div(index, per_w) == part)
            def _():
                cols = pl.ds(pl.multiple_of((index - part * per_w) * n_tile, n_tile), n_tile)
                getattr(pltpu.make_async_copy(w_ref.at[:, cols], w_buf.at[slot], w_sems.at[slot]), act)()

    @pl.when(step == 0)
    def _():
        fetch(step, 'start')
        copies = []
        first = 0
        for which, index in picks:
            src = rows_in[which]
            if index is not None:
                src = src.at[index * CP_SIZE + cp_ref[0]] if index < OWN else src.at[index - OWN]
            chunk = src.shape[0]
            copies.append((src, x_all.at[pl.ds(first, chunk), :]))
            first += chunk
        for copy in fetch_all(copies, x_sems):
            copy.wait()

    @pl.when(step < last)
    def _():
        fetch(step + 1, 'start')

    fetch(step, 'wait')
    out_ref[...] = jnp.dot(x_all[...], w_buf[lax.rem(step, 2)], preferred_element_type=jnp.float32).astype(jnp.bfloat16)


def project(cp_i, rows_in, picks, chunk, weights, n_tile=QKV_TILE):
    dim, width = weights[0].shape
    n_tile = min(n_tile, width)
    n_rows = len(picks) * chunk
    any_spec = pl.BlockSpec(memory_space=pl.ANY)
    return pl.pallas_call(
        functools.partial(qkv_kernel, len(rows_in), picks),
        out_shape=jax.ShapeDtypeStruct((n_rows, 3 * width), jnp.bfloat16),
        grid_spec=pltpu.PrefetchScalarGridSpec(
            num_scalar_prefetch=1, grid=(3 * width // n_tile,), in_specs=[any_spec] * (len(rows_in) + 3),
            out_specs=pl.BlockSpec((n_rows, n_tile), lambda g, cp_ref: (0, g)),
            scratch_shapes=[pltpu.VMEM((n_rows, dim), jnp.bfloat16), pltpu.VMEM((2, dim, n_tile), jnp.bfloat16),
                            pltpu.SemaphoreType.DMA((2,)), pltpu.SemaphoreType.DMA((len(picks),))]),
        compiler_params=pltpu.CompilerParams(dimension_semantics=('arbitrary',), vmem_limit_bytes=58 * 2 ** 20),
        cost_estimate=pl.CostEstimate(flops=6 * n_rows * dim * width, bytes_accessed=6 * dim * width + 2 * n_rows * (dim + 3 * width), transcendentals=0),
        name='project',
    )(cp_i, *rows_in, *weights)


def out_kernel(n_w, placed, part_w, cp_ref, *refs):
    w_refs, pieces = refs[:n_w], refs[n_w:n_w + len(placed)]
    add_ref = refs[n_w + len(placed)]
    out_ref, o_all, sems = refs[-3:]
    chunk, width = pieces[0].shape
    cp_i = cp_ref[0]

    @pl.when(pl.program_id(0) == 0)
    def _():
        copies = []
        for piece, (group, mc, first, split) in zip(pieces, placed):
            rows = pl.ds(pl.multiple_of((group * CP_SIZE + (cp_i ^ mc)) * chunk, chunk), chunk)
            if not split:
                copies.append((piece, o_all.at[rows, pl.ds(first, width)]))
                continue
            for part in range(CP_SIZE):
                cols = pl.ds(pl.multiple_of((cp_i ^ part) * part_w, part_w), part_w)
                copies.append((piece.at[:, cols], o_all.at[rows, pl.ds(first + part * part_w, part_w)]))
        for copy in fetch_all(copies, sems):
            copy.wait()

    first, acc = 0, None
    for w_ref in w_refs:
        depth = w_ref.shape[0]
        term = jnp.dot(o_all[:, first:first + depth], w_ref[...], preferred_element_type=jnp.float32)
        acc = term if acc is None else acc + term
        first += depth
    out_ref[...] = (add_ref[...].astype(jnp.float32) + acc).astype(out_ref.dtype)


def out_project(cp_i, w_parts, pieces, placed, addend, out_type, row_block, buf=None, n_tile=OUT_TILE):
    chunk, width = pieces[0].shape
    depth = sum(w.shape[0] for w in w_parts)
    n_rows = chunk * len(pieces) * width // depth
    dim = addend.shape[1]
    n_tile = min(n_tile, dim)
    any_spec = pl.BlockSpec(memory_space=pl.ANY)
    row_spec = pl.BlockSpec((n_rows, n_tile), lambda g, cp_ref: (row_block, g))
    operands = [*w_parts, *pieces, addend]
    in_specs = [pl.BlockSpec((w.shape[0], n_tile), lambda g, cp_ref: (0, g)) for w in w_parts] + [any_spec] * len(pieces) + [row_spec]
    aliases = {}
    if buf is not None:
        aliases = {1 + len(operands): 0}
        operands.append(buf)
        in_specs.append(any_spec)
    return pl.pallas_call(
        functools.partial(out_kernel, len(w_parts), placed, width // CP_SIZE),
        out_shape=out_type,
        grid_spec=pltpu.PrefetchScalarGridSpec(
            num_scalar_prefetch=1, grid=(dim // n_tile,), in_specs=in_specs, out_specs=row_spec,
            scratch_shapes=[pltpu.VMEM((n_rows, depth), jnp.bfloat16), pltpu.SemaphoreType.DMA((CP_SIZE * len(pieces),))]),
        input_output_aliases=aliases,
        compiler_params=pltpu.CompilerParams(dimension_semantics=('arbitrary',), vmem_limit_bytes=52 * 2 ** 20),
        cost_estimate=pl.CostEstimate(flops=2 * n_rows * depth * dim, bytes_accessed=2 * depth * dim + 2 * n_rows * (depth + 2 * dim), transcendentals=0),
        name='out_project',
    )(cp_i, *operands)


def solution(mesh):
    cp_size, tp_size = mesh.shape['cp'], mesh.shape['tp']
    n_peers = cp_size * tp_size
    row_spec = P('data', ('cp', 'tp'))

    def swap(vals, m):
        if not m:
            return vals
        mc, mt = m // tp_size, m % tp_size
        pairs = [(t * cp_size + c, (t ^ mt) * cp_size + (c ^ mc)) for t in range(tp_size) for c in range(cp_size)]
        return lax.ppermute(vals, ('tp', 'cp'), pairs)

    def local_fn(x_rows, pos_rows, w_query, w_key, w_value, w_out):
        n_seqs, chunk, dim = x_rows.shape
        n_own = n_seqs // cp_size
        cp_i, tp_i = lax.axis_index('cp'), lax.axis_index('tp')
        me = cp_i * tp_size + tp_i
        peers = me ^ jnp.arange(n_peers, dtype=jnp.int32)
        peer_cp, peer_tp = peers // tp_size, peers % tp_size
        block_of = jnp.where(peer_tp == 0, peer_cp, 2 * cp_size - 1 - peer_cp)
        chunk_of = jnp.argmax(block_of[None, :] == jnp.arange(n_peers, dtype=jnp.int32)[:, None], axis=1).astype(jnp.int32)
        place = jnp.stack([block_of, chunk_of]).astype(jnp.int32)
        pos_all = lax.all_gather(pos_rows, ('tp', 'cp'), axis=0, tiled=False)
        pos_all = jnp.take(pos_all, peer_tp * cp_size + peer_cp, axis=0)
        cp_ref = cp_i.reshape(1).astype(jnp.int32)
        weights = (w_query, w_key, w_value)
        far = [m for m in range(n_peers) if m not in NEAR]

        def seq_of(s, mc):
            return s * cp_size + (cp_i ^ mc)

        def rows_for(s, mc):
            return lax.dynamic_index_in_dim(x_rows, seq_of(s, mc), 0, keepdims=False)

        near_got = swap(jnp.stack([rows_for(s, 1) for s in range(n_own)]), NEAR[1])
        far_got = []
        for s in range(n_own):
            outgoing = [rows_for(s, mc) for mc in range(cp_size)]
            far_got.append([swap(outgoing[m // tp_size], m) for m in far])

        q_rows = w_out.shape[0] // cp_size
        piece_rows = q_rows // W_PIECES
        w_got = [[None] * W_PIECES for _ in range(cp_size)]
        for p in range(W_PIECES):
            mine = lax.dynamic_slice_in_dim(w_out, cp_i * q_rows + p * piece_rows, piece_rows, 0)
            w_got[0][p] = swap(mine, 1)
            w_got[1][p] = swap(w_got[0][p], tp_size)
            w_got[2][p] = swap(w_got[0][p], 2 * tp_size)
            w_got[3][p] = swap(w_got[2][p], tp_size)
        w_other = [piece for part in w_got for piece in part]

        picks = tuple(pick for s in range(n_own) for pick in ((0, s), (1, OWN + s)))
        qkv_near = project(cp_ref, [x_rows, near_got], picks, chunk, weights)
        o_got = []
        for s in range(n_own):
            pos_seq = lax.dynamic_index_in_dim(pos_all, seq_of(s, 0), 1, keepdims=False).reshape(-1)
            cos_t, sin_t = rope_tables(pos_seq)
            qkv_far = project(cp_ref, far_got[s], tuple((n, None) for n in range(len(far))), chunk, weights)
            o = attend(place, qkv_near, qkv_far, s, NEAR, cos_t, sin_t)
            got = []
            for m in range(n_peers):
                got.append(swap(o[m], m))
            o_got.append(got)

        x_flat = x_rows.reshape(n_seqs * chunk, dim)
        early = n_own - 1
        width = w_out.shape[0]
        y_type = jax.ShapeDtypeStruct(x_flat.shape, jnp.bfloat16)
        part_type = jax.ShapeDtypeStruct((early * cp_size * chunk, dim), jnp.float32)
        placed = [(s, mc, 0, False) for s in range(early) for mc in range(cp_size)]
        partial = out_project(cp_ref, [w_out], [o_got[s][mc * tp_size] for s, mc, _, _ in placed], placed, x_flat, part_type, 0)
        placed = [(s, mc, 0, True) for s in range(early) for mc in range(cp_size)]
        y = out_project(cp_ref, w_other, [o_got[s][mc * tp_size + 1] for s, mc, _, _ in placed], placed, partial, y_type, 0)
        placed = [(0, m // tp_size, (m % tp_size) * width, bool(m % tp_size)) for m in range(n_peers)]
        y = out_project(cp_ref, [w_out] + w_other, o_got[early], placed, x_flat, y_type, early, y)
        return y.reshape(n_seqs, chunk, dim)


    return jax.shard_map(local_fn, mesh=mesh,
                         in_specs=(row_spec, row_spec, P(None, 'tp'), P(None, 'tp'), P(None, 'tp'), P('tp', None)),
                         out_specs=row_spec, check_vma=False)
```

```python
import functools
import math
import jax
import jax.numpy as jnp
from jax import lax
from jax.experimental import pallas as pl
from jax.experimental.pallas import tpu as pltpu
from jax.sharding import PartitionSpec as P

HEAD_DIM = 128
ROPE_BASE = 500000
Q_TILE = 256
STEP_HEADS = 4
EXP_SCALE = math.log2(math.e) / math.sqrt(HEAD_DIM)
W_PIECES = 4
QKV_TILE = 512
OUT_TILE = 512
CP_SIZE = 4
NEAR = (0, 2)


def rope_tables(pos_vals):
    inv_freq = jnp.asarray([ROPE_BASE ** (-2.0 * freq_idx / HEAD_DIM) for freq_idx in range(HEAD_DIM // 2)], dtype=jnp.float32)
    angles = pos_vals.astype(jnp.float32)[..., None] * inv_freq
    cos_t, sin_t = jnp.cos(angles), jnp.sin(angles)
    return jnp.concatenate([cos_t, cos_t], axis=-1), jnp.concatenate([-sin_t, sin_t], axis=-1)


def attend_kernel(sources, place_ref, *refs):
    n_chunks = place_ref.shape[1]
    qkv_refs, (cos_ref, sin_ref) = refs[:6], refs[6:8]
    o_refs, (q_seq, k_seq, v_seq, o_seq) = refs[8:8 + n_chunks], refs[8 + n_chunks:]
    n_rows, step_w = q_seq.shape
    chunk = n_rows // n_chunks
    heads = [slice(h * HEAD_DIM, (h + 1) * HEAD_DIM) for h in range(step_w // HEAD_DIM)]
    for m, (which, first) in enumerate(sources):
        q_ref, k_ref, v_ref = qkv_refs[which::2]
        src, tab = slice(first, first + chunk), slice(m * chunk, (m + 1) * chunk)
        dst = pl.ds(pl.multiple_of(place_ref[0, m] * chunk, chunk), chunk)
        cos_t, sin_t = cos_ref[tab, :], sin_ref[tab, :]
        for cols in heads:
            for in_ref, out_ref in ((q_ref, q_seq), (k_ref, k_seq)):
                vals = in_ref[src, cols].astype(jnp.float32)
                out_ref[dst, cols] = (vals * cos_t + pltpu.roll(vals, HEAD_DIM // 2, 1) * sin_t).astype(jnp.bfloat16)
        v_seq[dst, :] = v_ref[src, :]
    tile = min(Q_TILE, n_rows)
    below = lax.broadcasted_iota(jnp.int32, (tile, tile), 1) <= lax.broadcasted_iota(jnp.int32, (tile, tile), 0)
    contract_last = (((1,), (1,)), ((), ()))
    for j in range(n_rows // tile):
        for cols in heads:
            here = slice(j * tile, (j + 1) * tile)
            q_tile = q_seq[here, cols]
            s_diag = lax.dot_general(q_tile, k_seq[here, cols], contract_last, preferred_element_type=jnp.float32)
            s_diag = jnp.where(below, s_diag, -jnp.inf)
            row_max = jnp.max(s_diag, axis=1, keepdims=True)
            if j:
                s_prev = lax.dot_general(q_tile, k_seq[:j * tile, cols], contract_last, preferred_element_type=jnp.float32)
                row_max = jnp.maximum(row_max, jnp.max(s_prev, axis=1, keepdims=True))
            p_diag = jnp.exp2((s_diag - row_max) * EXP_SCALE)
            row_sum = jnp.sum(p_diag, axis=1, keepdims=True)
            acc = jnp.dot(p_diag.astype(jnp.bfloat16), v_seq[here, cols], preferred_element_type=jnp.float32)
            if j:
                p_prev = jnp.exp2((s_prev - row_max) * EXP_SCALE)
                row_sum = row_sum + jnp.sum(p_prev, axis=1, keepdims=True)
                acc = acc + jnp.dot(p_prev.astype(jnp.bfloat16), v_seq[:j * tile, cols], preferred_element_type=jnp.float32)
            o_seq[here, cols] = (acc / row_sum).astype(jnp.bfloat16)
    for m, o_ref in enumerate(o_refs):
        o_ref[...] = o_seq[pl.ds(pl.multiple_of(place_ref[0, m] * chunk, chunk), chunk), :]


def attend(place, qkv_near, qkv_far, s, near, cos_t, sin_t):
    n_rows, n_peers = cos_t.shape[0], place.shape[1]
    chunk = n_rows // n_peers
    width = qkv_far.shape[1] // 3
    step_w = STEP_HEADS * HEAD_DIM
    steps = width // step_w
    near_rows = len(near) * chunk
    far = [m for m in range(n_peers) if m not in near]
    sources = [(0, near.index(m) * chunk) if m in near else (1, far.index(m) * chunk) for m in range(n_peers)]
    qkv_specs = []
    for part in range(3):
        qkv_specs.append(pl.BlockSpec((near_rows, step_w), lambda g, place_ref, part=part: (s, part * steps + g)))
        qkv_specs.append(pl.BlockSpec((len(far) * chunk, step_w), lambda g, place_ref, part=part: (0, part * steps + g)))
    table_spec = pl.BlockSpec((n_rows, HEAD_DIM), lambda g, place_ref: (0, 0))
    out_spec = pl.BlockSpec((chunk, step_w), lambda g, place_ref: (0, g))
    flops = 2 * n_rows * n_rows * width
    return pl.pallas_call(
        functools.partial(attend_kernel, sources),
        out_shape=[jax.ShapeDtypeStruct((chunk, width), jnp.bfloat16)] * n_peers,
        grid_spec=pltpu.PrefetchScalarGridSpec(
            num_scalar_prefetch=1, grid=(steps,),
            in_specs=qkv_specs + [table_spec] * 2, out_specs=[out_spec] * n_peers,
            scratch_shapes=[pltpu.VMEM((n_rows, step_w), jnp.bfloat16)] * 4),
        compiler_params=pltpu.CompilerParams(dimension_semantics=('arbitrary',), vmem_limit_bytes=48 * 2 ** 20),
        cost_estimate=pl.CostEstimate(flops=4 * flops, bytes_accessed=8 * n_rows * width, transcendentals=n_rows * n_rows * width // HEAD_DIM // 2),
        name='attend',
    )(place, *[qkv_near, qkv_far] * 3, cos_t, sin_t)


def fetch_all(copies, sems):
    copies = [pltpu.make_async_copy(src, dst, sems.at[n]) for n, (src, dst) in enumerate(copies)]
    for copy in copies:
        copy.start()
    return copies


def qkv_kernel(n_rows_in, picks, cp_ref, *refs):
    rows_in, w_refs = refs[:n_rows_in], refs[n_rows_in:n_rows_in + 3]
    out_ref, x_all, w_buf, w_sems, x_sems = refs[n_rows_in + 3:]
    step, last = pl.program_id(0), pl.num_programs(0) - 1
    n_tile = w_buf.shape[2]
    per_w = w_refs[0].shape[1] // n_tile

    def fetch(index, act):
        slot = lax.rem(index, 2)
        for part, w_ref in enumerate(w_refs):
            @pl.when(lax.div(index, per_w) == part)
            def _():
                cols = pl.ds(pl.multiple_of((index - part * per_w) * n_tile, n_tile), n_tile)
                getattr(pltpu.make_async_copy(w_ref.at[:, cols], w_buf.at[slot], w_sems.at[slot]), act)()

    @pl.when(step == 0)
    def _():
        fetch(step, 'start')
        copies = []
        first = 0
        for which, index in picks:
            src = rows_in[which]
            if index is not None:
                src = src.at[index * CP_SIZE + cp_ref[0]]
            chunk = src.shape[0]
            copies.append((src, x_all.at[pl.ds(first, chunk), :]))
            first += chunk
        for copy in fetch_all(copies, x_sems):
            copy.wait()

    @pl.when(step < last)
    def _():
        fetch(step + 1, 'start')

    fetch(step, 'wait')
    out_ref[...] = jnp.dot(x_all[...], w_buf[lax.rem(step, 2)], preferred_element_type=jnp.float32).astype(jnp.bfloat16)


def project(cp_i, rows_in, picks, chunk, weights, n_tile=QKV_TILE):
    dim, width = weights[0].shape
    n_tile = min(n_tile, width)
    n_rows = len(picks) * chunk
    any_spec = pl.BlockSpec(memory_space=pl.ANY)
    return pl.pallas_call(
        functools.partial(qkv_kernel, len(rows_in), picks),
        out_shape=jax.ShapeDtypeStruct((n_rows, 3 * width), jnp.bfloat16),
        grid_spec=pltpu.PrefetchScalarGridSpec(
            num_scalar_prefetch=1, grid=(3 * width // n_tile,), in_specs=[any_spec] * (len(rows_in) + 3),
            out_specs=pl.BlockSpec((n_rows, n_tile), lambda g, cp_ref: (0, g)),
            scratch_shapes=[pltpu.VMEM((n_rows, dim), jnp.bfloat16), pltpu.VMEM((2, dim, n_tile), jnp.bfloat16),
                            pltpu.SemaphoreType.DMA((2,)), pltpu.SemaphoreType.DMA((len(picks),))]),
        compiler_params=pltpu.CompilerParams(dimension_semantics=('arbitrary',), vmem_limit_bytes=58 * 2 ** 20),
        cost_estimate=pl.CostEstimate(flops=6 * n_rows * dim * width, bytes_accessed=6 * dim * width + 2 * n_rows * (dim + 3 * width), transcendentals=0),
        name='project',
    )(cp_i, *rows_in, *weights)


def out_kernel(n_w, placed, part_w, cp_ref, *refs):
    w_refs, pieces = refs[:n_w], refs[n_w:n_w + len(placed)]
    add_ref = refs[n_w + len(placed)]
    out_ref, o_all, sems = refs[-3:]
    chunk, width = pieces[0].shape
    cp_i = cp_ref[0]

    @pl.when(pl.program_id(0) == 0)
    def _():
        copies = []
        for piece, (group, mc, first, split) in zip(pieces, placed):
            rows = pl.ds(pl.multiple_of((group * CP_SIZE + (cp_i ^ mc)) * chunk, chunk), chunk)
            if not split:
                copies.append((piece, o_all.at[rows, pl.ds(first, width)]))
                continue
            for part in range(CP_SIZE):
                cols = pl.ds(pl.multiple_of((cp_i ^ part) * part_w, part_w), part_w)
                copies.append((piece.at[:, cols], o_all.at[rows, pl.ds(first + part * part_w, part_w)]))
        for copy in fetch_all(copies, sems):
            copy.wait()

    first, acc = 0, None
    for w_ref in w_refs:
        depth = w_ref.shape[0]
        term = jnp.dot(o_all[:, first:first + depth], w_ref[...], preferred_element_type=jnp.float32)
        acc = term if acc is None else acc + term
        first += depth
    out_ref[...] = (add_ref[...].astype(jnp.float32) + acc).astype(out_ref.dtype)


def out_project(cp_i, w_parts, pieces, placed, addend, out_type, row_block, buf=None, n_tile=OUT_TILE, add_block=None):
    chunk, width = pieces[0].shape
    depth = sum(w.shape[0] for w in w_parts)
    n_rows = chunk * len(pieces) * width // depth
    dim = addend.shape[1]
    n_tile = min(n_tile, dim)
    any_spec = pl.BlockSpec(memory_space=pl.ANY)
    add_block = row_block if add_block is None else add_block
    row_spec = pl.BlockSpec((n_rows, n_tile), lambda g, cp_ref: (row_block, g))
    add_spec = pl.BlockSpec((n_rows, n_tile), lambda g, cp_ref: (add_block, g))
    operands = [*w_parts, *pieces, addend]
    in_specs = [pl.BlockSpec((w.shape[0], n_tile), lambda g, cp_ref: (0, g)) for w in w_parts] + [any_spec] * len(pieces) + [add_spec]
    aliases = {}
    if buf is not None:
        aliases = {1 + len(operands): 0}
        operands.append(buf)
        in_specs.append(any_spec)
    return pl.pallas_call(
        functools.partial(out_kernel, len(w_parts), placed, width // CP_SIZE),
        out_shape=out_type,
        grid_spec=pltpu.PrefetchScalarGridSpec(
            num_scalar_prefetch=1, grid=(dim // n_tile,), in_specs=in_specs, out_specs=row_spec,
            scratch_shapes=[pltpu.VMEM((n_rows, depth), jnp.bfloat16), pltpu.SemaphoreType.DMA((CP_SIZE * len(pieces),))]),
        input_output_aliases=aliases,
        compiler_params=pltpu.CompilerParams(dimension_semantics=('arbitrary',), vmem_limit_bytes=52 * 2 ** 20),
        cost_estimate=pl.CostEstimate(flops=2 * n_rows * depth * dim, bytes_accessed=2 * depth * dim + 2 * n_rows * (depth + 2 * dim), transcendentals=0),
        name='out_project',
    )(cp_i, *operands)


def solution(mesh):
    cp_size, tp_size = mesh.shape['cp'], mesh.shape['tp']
    n_peers = cp_size * tp_size
    row_spec = P('data', ('cp', 'tp'))

    def swap(vals, m):
        if not m:
            return vals
        mc, mt = m // tp_size, m % tp_size
        pairs = [(t * cp_size + c, (t ^ mt) * cp_size + (c ^ mc)) for t in range(tp_size) for c in range(cp_size)]
        return lax.ppermute(vals, ('tp', 'cp'), pairs)

    def local_fn(x_rows, pos_rows, w_query, w_key, w_value, w_out):
        n_seqs, chunk, dim = x_rows.shape
        n_own = n_seqs // cp_size
        cp_i, tp_i = lax.axis_index('cp'), lax.axis_index('tp')
        me = cp_i * tp_size + tp_i
        peers = me ^ jnp.arange(n_peers, dtype=jnp.int32)
        peer_cp, peer_tp = peers // tp_size, peers % tp_size
        block_of = jnp.where(peer_tp == 0, peer_cp, 2 * cp_size - 1 - peer_cp)
        chunk_of = jnp.argmax(block_of[None, :] == jnp.arange(n_peers, dtype=jnp.int32)[:, None], axis=1).astype(jnp.int32)
        place = jnp.stack([block_of, chunk_of]).astype(jnp.int32)
        pos_all = lax.all_gather(pos_rows, ('tp', 'cp'), axis=0, tiled=False)
        pos_all = jnp.take(pos_all, peer_tp * cp_size + peer_cp, axis=0)
        cp_ref = cp_i.reshape(1).astype(jnp.int32)
        weights = (w_query, w_key, w_value)
        far = [m for m in range(n_peers) if m not in NEAR]

        def seq_of(s, mc):
            return s * cp_size + (cp_i ^ mc)

        far_got, near_got, x_src = [], [], x_rows
        for s in range(n_own):
            outgoing = [lax.dynamic_index_in_dim(x_src, seq_of(s, mc), 0, keepdims=False) for mc in range(cp_size)]
            near_out = [lax.dynamic_index_in_dim(x_rows, seq_of(n, 1), 0, keepdims=False) for n in range(n_own)] if s == 0 else []
            x_src = lax.optimization_barrier((x_rows, *outgoing))[0]
            if s == 0:
                near_got = [swap(rows, NEAR[1]) for rows in near_out]
            far_got.append([swap(outgoing[m // tp_size], m) for m in far])

        q_rows = w_out.shape[0] // cp_size
        piece_rows = q_rows // W_PIECES
        w_got = [[None] * W_PIECES for _ in range(cp_size)]
        for p in range(W_PIECES):
            mine = lax.dynamic_slice_in_dim(w_out, cp_i * q_rows + p * piece_rows, piece_rows, 0)
            w_got[0][p] = swap(mine, 1)
            w_got[1][p] = swap(w_got[0][p], tp_size)
            w_got[2][p] = swap(w_got[0][p], 2 * tp_size)
            w_got[3][p] = swap(w_got[2][p], tp_size)
        w_other = [piece for part in w_got for piece in part]

        picks = tuple(pick for s in range(n_own) for pick in ((0, s), (1 + s, None)))
        qkv_near = project(cp_ref, [x_rows] + near_got, picks, chunk, weights)
        o_got = []
        for s in range(n_own):
            pos_seq = lax.dynamic_index_in_dim(pos_all, seq_of(s, 0), 1, keepdims=False).reshape(-1)
            cos_t, sin_t = rope_tables(pos_seq)
            qkv_far = project(cp_ref, far_got[s], tuple((n, None) for n in range(len(far))), chunk, weights)
            o = attend(place, qkv_near, qkv_far, s, NEAR, cos_t, sin_t)
            got = []
            for m in range(n_peers):
                got.append(swap(o[m], m))
            o_got.append(got)

        x_flat = x_rows.reshape(n_seqs * chunk, dim)
        early = n_own - 1
        y_type = jax.ShapeDtypeStruct(x_flat.shape, jnp.bfloat16)
        part_type = jax.ShapeDtypeStruct((early * cp_size * chunk, dim), jnp.float32)
        placed = [(s, mc, 0, False) for s in range(early) for mc in range(cp_size)]
        partial = out_project(cp_ref, [w_out], [o_got[s][mc * tp_size] for s, mc, _, _ in placed], placed, x_flat, part_type, 0)
        placed = [(s, mc, 0, True) for s in range(early) for mc in range(cp_size)]
        y = out_project(cp_ref, w_other, [o_got[s][mc * tp_size + 1] for s, mc, _, _ in placed], placed, partial, y_type, 0)
        last_type = jax.ShapeDtypeStruct((cp_size * chunk, dim), jnp.float32)
        placed = [(0, mc, 0, False) for mc in range(cp_size)]
        partial = out_project(cp_ref, [w_out], o_got[early][0::tp_size], placed, x_flat, last_type, 0, add_block=early)
        placed = [(0, mc, 0, True) for mc in range(cp_size)]
        y = out_project(cp_ref, w_other, o_got[early][1::tp_size], placed, partial, y_type, early, y, add_block=0)
        return y.reshape(n_seqs, chunk, dim)


    return jax.shard_map(local_fn, mesh=mesh,
                         in_specs=(row_spec, row_spec, P(None, 'tp'), P(None, 'tp'), P(None, 'tp'), P('tp', None)),
                         out_specs=row_spec, check_vma=False)
```
